32 devices in a mesh: gy: 4 (over y, x), gx: 8 (over z, core).
Axes of the slice: x: 2, y: 2, z: 4, core: 2. Of those that a mesh axis runs over, the one named last changes fastest.
Arguments:
- u_field: float32 [8, 512, 1024], P(None, 'gx', 'gy')
- v_field: float32 [8, 512, 1024], P(None, 'gx', 'gy')
- w_field: float32 [8, 512, 1024], P(None, 'gx', 'gy')
- sep_x: int32 [16], replicated, may hold values from 1 to 128, as said below
- sep_y: int32 [16], replicated, may hold values from 1 to 256, as said below
- sep_z: int32 [16], replicated, may hold values from 1 to 4
Outputs:
- correlation: float32 [3, 16], replicated
The draws below stay inside these ranges and needn't reach their ends.
Inputs may be any that keep to these rules, and one draw needn't show every extreme that they name: `sep_x`: every separation along x lies in 1 to 128, and 128 is among them in every draw; repeats may occur. `sep_y`: every separation along y lies in 1 to 256, and 256 is among them in every draw; repeats may occur.
All inputs are finite; a program needn't handle non-finite values.
Results may differ from the reference program's by a relative error of at most 0.0003.
Values sent between devices are 32-bit elements; how exact they have to be, the bound alone decides.
A program may use at most 64 MiB of HBM per device.

```python
import math
import jax
import jax.numpy as jnp
from jax import lax

PLANES = 8
CX = 64
CY = 256
SEPS = 16
NX = 512
NY = 1024


def rough_scale(key, shape, spread):
    return jnp.exp(jax.random.uniform(key, shape, jnp.float32, -spread, spread))


def smooth_field(key, salt_value):
    key = jax.random.fold_in(key, salt_value)
    key_list = jax.random.split(key, 12)
    mode_count = 6
    plane_pos = jnp.arange(PLANES, dtype=jnp.float32)[:, None, None]
    row_pos = jnp.arange(NX, dtype=jnp.float32)[None, :, None]
    column_pos = jnp.arange(NY, dtype=jnp.float32)[None, None, :]
    wave_x = jax.random.randint(key_list[0], (mode_count,), 1, 5).astype(jnp.float32)
    wave_y = jax.random.randint(key_list[1], (mode_count,), 1, 5).astype(jnp.float32)
    wave_z = jax.random.randint(key_list[2], (mode_count,), 0, 3).astype(jnp.float32)
    phases = jax.random.uniform(key_list[3], (mode_count, 3), jnp.float32, 0.0, 2.0 * math.pi)
    amplitude = jax.random.uniform(key_list[4], (mode_count,), jnp.float32, 0.5, 1.0)
    smooth = jnp.zeros((PLANES, NX, NY), jnp.float32)
    for mode_index in range(mode_count):
        cos_x = jnp.cos(2.0 * math.pi * wave_x[mode_index] * row_pos / NX + phases[mode_index, 0])
        cos_y = jnp.cos(2.0 * math.pi * wave_y[mode_index] * column_pos / NY + phases[mode_index, 1])
        cos_z = jnp.cos(2.0 * math.pi * wave_z[mode_index] * plane_pos / (4.0 * PLANES) + phases[mode_index, 2])
        smooth = smooth + amplitude[mode_index] * cos_x * cos_y * cos_z
    spread = 1.15
    noise_part = 0.7 * jax.random.normal(key_list[11], (PLANES, NX, NY), jnp.float32)
    smooth_scale = rough_scale(key_list[5], (PLANES, 1, 1), spread) * rough_scale(key_list[6], (1, NX, 1), spread) * rough_scale(key_list[7], (1, 1, NY), spread)
    noise_scale = rough_scale(key_list[8], (PLANES, 1, 1), spread) * rough_scale(key_list[9], (1, NX, 1), spread) * rough_scale(key_list[10], (1, 1, NY), spread)
    return smooth_scale * (1.5 * smooth) + noise_scale * noise_part


def draw_u_field(key, part):
    return smooth_field(key, 11)


def draw_v_field(key, part):
    return smooth_field(key, 23)


def draw_w_field(key, part):
    return smooth_field(key, 37)


def separations(key, salt_value, largest):
    key = jax.random.fold_in(key, salt_value)
    key_list = jax.random.split(key, 2)
    others = jax.random.randint(key_list[0], (SEPS - 1,), 1, largest + 1)
    values = jnp.concatenate([others, jnp.full((1,), largest, jnp.int32)])
    return jax.random.permutation(key_list[1], values).astype(jnp.int32)


def draw_sep_x(key, part):
    return separations(key, 41, 2 * CX)


def draw_sep_y(key, part):
    return separations(key, 53, CY)


def touch_ends(drawn, stream_key, smallest, top_value):
    dims = drawn.shape
    index_at = [jax.random.randint(jax.random.fold_in(stream_key, axis), (), 0, dims[axis]) for axis in range(len(dims))]
    drawn = drawn.at[tuple(index_at)].set(smallest)
    longest = dims.index(max(dims))
    index_at[longest] = (index_at[longest] + 1) % dims[longest]
    return drawn.at[tuple(index_at)].set(top_value)


def setup_inputs(seed: int = 0) -> dict:
    streams_of = jax.random.split(jax.random.key(seed), 7)
    u_field = draw_u_field(jax.random.fold_in(streams_of[6], 71), 0)
    v_field = draw_v_field(jax.random.fold_in(streams_of[6], 71), 0)
    w_field = draw_w_field(jax.random.fold_in(streams_of[6], 71), 0)
    sep_x = draw_sep_x(jax.random.fold_in(streams_of[6], 71), 0)
    sep_y = draw_sep_y(jax.random.fold_in(streams_of[6], 71), 0)
    sep_z = touch_ends(jax.random.randint(streams_of[5], (SEPS,), 1, PLANES // 2 + 1), jax.random.fold_in(streams_of[5], 1), 1, (PLANES // 2 + 1) - 1).astype(jnp.int32)
    return {"u_field": u_field, "v_field": v_field, "w_field": w_field, "sep_x": sep_x, "sep_y": sep_y, "sep_z": sep_z}


def reference(u_field, v_field, w_field, sep_x, sep_y, sep_z):
    planes = u_field.shape[0]

    def along_x(lag_value):
        return jnp.sum(u_field * jnp.roll(u_field, -lag_value, axis=1))

    def along_y(lag_value):
        return jnp.sum(v_field * jnp.roll(v_field, -lag_value, axis=2))

    padded = jnp.concatenate([w_field, jnp.zeros_like(w_field)], axis=0)

    def along_z(lag_value):
        shifted = lax.dynamic_slice_in_dim(padded, lag_value.astype(jnp.int32), planes, 0)
        return jnp.sum(w_field * shifted)

    sums_x = lax.map(along_x, sep_x)
    sums_y = lax.map(along_y, sep_y)
    sums_z = lax.map(along_z, sep_z)
    energy_u = jnp.sum(u_field * u_field)
    energy_v = jnp.sum(v_field * v_field)
    energy_w = jnp.sum(w_field * w_field)
    factor = jnp.float32(planes) / (jnp.float32(planes) - sep_z.astype(jnp.float32))
    row_x = sums_x / energy_u
    row_y = sums_y / energy_v
    row_z = sums_z / energy_w * factor
    return jnp.stack([row_x, row_y, row_z], axis=0)
```

```python
import functools

import jax
import jax.numpy as jnp
from jax import lax
from jax.experimental import pallas as pl
from jax.experimental.pallas import tpu as pltpu
from jax.sharding import PartitionSpec as P

MESH = pl.DeviceIdType.MESH
LANES = 128
FIELD_LANES = 32


def split(value):
    high = value.astype(jnp.bfloat16)
    low = (value - high.astype(jnp.float32)).astype(jnp.bfloat16)
    return high, low


def product(left, right, dims):
    dot = functools.partial(
        lax.dot_general, dimension_numbers=(dims, ((), ())), preferred_element_type=jnp.float32
    )
    return dot(left[0], right[0]) + (dot(left[0], right[1]) + dot(left[1], right[0]))


def lag_sums(gram, lags, largest):
    rows = gram.shape[0]
    window = largest + LANES
    folded = gram[:LANES, :window]
    for start in range(LANES, rows, LANES):
        folded = folded + gram[start : start + LANES, start : start + window]
    at = jnp.broadcast_to(lags, (8, LANES)) + lax.broadcasted_iota(jnp.int32, (8, LANES), 0)
    total = None
    for start in range(0, LANES, 8):
        index = at + start
        lane, tile = index & (LANES - 1), index // LANES
        part = None
        for column in range(0, window, LANES):
            piece = jnp.take_along_axis(folded[start : start + 8, column : column + LANES], lane, axis=1)
            part = piece if part is None else jnp.where(tile == column // LANES, piece, part)
        total = part if total is None else total + part
    return jnp.where(lags < 0, 0.0, jnp.sum(total, axis=0, keepdims=True))


def kernel(
    n_gx, n_gy,
    u_hbm, v_hbm, w_hbm, sep_x_hbm, sep_y_hbm, sep_z_hbm, out_ref,
    u_own, v_own, w_own, u_wide, v_wide, sep_s, rows,
    plane_sem, load_sem, sep_sem, send_sem, u_recv, recv_sem, row_sem, line_sem, pair_sem,
):
    planes, width_x, width_y = v_own.shape
    seps = sep_s.shape[1]
    quarter, half = planes // 4, planes // 2
    gx, gy = lax.axis_index("gx"), lax.axis_index("gy")
    core, parity = lax.rem(gx, 2), lax.rem(gy, 2)
    chip_first = gx - core

    load_u = [
        pltpu.make_async_copy(u_hbm.at[item], u_own.at[item], plane_sem.at[item])
        for item in range(quarter)
    ]
    load_v = pltpu.make_async_copy(v_hbm, v_own, load_sem.at[0])
    load_w = pltpu.make_async_copy(w_hbm, w_own, load_sem.at[1])
    for copy in load_u:
        copy.start()
    load_v.start()

    chip, chips = gx // 2, n_gx // 2
    first, last = chip == 0, chip == chips - 1
    near = gy + 1 - 2 * parity
    far_to = lax.rem(gy + n_gy - 2 + 4 * parity, n_gy)
    far_from = lax.rem(gy + n_gy + 2 - 4 * parity, n_gy)
    barrier = pltpu.get_barrier_semaphore()

    def greet(semaphore, **device):
        pl.semaphore_signal(semaphore, inc=1, device_id=device, device_id_type=MESH)

    @pl.when(~first)
    def _():
        greet(barrier, gx=chip_first - 2)
        greet(barrier, gx=chip_first - 1)

    @pl.when(~last)
    def _():
        greet(barrier, gx=chip_first + 2)
        greet(barrier, gx=chip_first + 3)

    greet(barrier, gx=chip_first + 1 - core)
    greet(barrier, gy=near)
    greet(barrier, gy=far_from)
    load_w.start()
    sep_loads = [
        pltpu.make_async_copy(ref, sep_s.at[index], sep_sem.at[0])
        for index, ref in enumerate((sep_x_hbm, sep_y_hbm, sep_z_hbm))
    ]
    places = []
    for side in range(2):
        places.append(pltpu.make_async_copy(
            u_hbm.at[:, side, core],
            u_wide.at[side, :, 2 * side + core],
            load_sem.at[2],
        ))
    places.append(pltpu.make_async_copy(
        v_hbm.at[pl.ds(half * parity, half)], v_wide.at[2 * parity], load_sem.at[2]
    ))
    for copy in places + sep_loads:
        copy.start()

    u_copies = {}
    for item in range(quarter):
        for other in range(2):
            for side in range(2):
                target = lax.rem(chip_first + (n_gx - 2 if side == 0 else 2), n_gx)
                u_copies[side, item, other] = (pltpu.make_async_remote_copy(
                    src_ref=u_own.at[item, side, other],
                    dst_ref=u_wide.at[side, item, (2 if side == 0 else 0) + core],
                    send_sem=send_sem.at[0],
                    recv_sem=u_recv.at[side, item],
                    device_id={"gx": target + other},
                    device_id_type=MESH,
                ))
    d_copies = []
    for side in range(2):
        d_copies.append(pltpu.make_async_remote_copy(
            src_ref=u_own.at[:, side, 1 - core],
            dst_ref=u_wide.at[side, :, 2 * side + core],
            send_sem=send_sem.at[2],
            recv_sem=recv_sem.at[0],
            device_id={"gx": chip_first + 1 - core},
            device_id_type=MESH,
        ))
    v_copies = []
    for item in range(half):
        v_copies.append(pltpu.make_async_remote_copy(
            src_ref=v_own.at[half * (1 - parity) + item],
            dst_ref=v_wide.at[1, item],
            send_sem=send_sem.at[1],
            recv_sem=recv_sem.at[1],
            device_id={"gy": near},
            device_id_type=MESH,
        ))
        v_copies.append(pltpu.make_async_remote_copy(
            src_ref=v_own.at[half * parity + item],
            dst_ref=v_wide.at[2 - 2 * parity, item],
            send_sem=send_sem.at[1],
            recv_sem=recv_sem.at[1],
            device_id={"gy": far_to},
            device_id_type=MESH,
        ))

    load_u[0].wait()
    inner = jnp.where(first, 0, 2) + jnp.where(last, 0, 2)
    pl.semaphore_wait(barrier, inner + 3)

    def start_u(side, items, at_end):
        wraps = first if side == 0 else last

        @pl.when(wraps if at_end else ~wraps)
        def _():
            for item in items:
                for other in range(2):
                    u_copies[side, item, other].start()

    ends = first | last
    for side in range(2):
        start_u(side, range(1), False)
    for copy in load_u[1:]:
        copy.wait()
    @pl.when(~ends)
    def _():
        for side in range(2):
            for item in range(1, quarter):
                for other in range(2):
                    u_copies[side, item, other].start()
    load_v.wait()
    for copy in v_copies + d_copies:
        copy.start()

    up, down = line_sem.at[0], line_sem.at[1]

    @pl.when(chip == 1)
    def _():
        greet(up, gx=gx + 2)

    @pl.when(chip == chips - 2)
    def _():
        greet(down, gx=gx - 2)

    @pl.when(chip >= 2)
    def _():
        pl.semaphore_wait(up, 1)

    @pl.when((chip >= 2) & (chip <= chips - 2))
    def _():
        greet(up, gx=gx + 2)

    @pl.when(chip <= chips - 3)
    def _():
        pl.semaphore_wait(down, 1)

    @pl.when((chip >= 1) & (chip <= chips - 3))
    def _():
        greet(down, gx=gx - 2)

    for side in range(2):
        start_u(side, range(quarter), True)
    @pl.when(ends)
    def _():
        for side in range(2):
            start_u(side, range(1, quarter), False)

    greet(pair_sem.at[0], gy=near)
    pl.semaphore_wait(pair_sem.at[0], 1)
    for hop in range(1, n_gy // 2):
        greet(pair_sem.at[hop], gy=far_from)
        pl.semaphore_wait(pair_sem.at[hop], 1)

    pltpu.make_async_copy(sep_s, sep_s, sep_sem.at[0]).wait()
    lane = lax.broadcasted_iota(jnp.int32, (1, LANES), 1)
    lag_row = jnp.full((1, LANES), -1, jnp.int32)
    for field in range(3):
        for index in range(seps):
            lag_row = jnp.where(lane == FIELD_LANES * field + index, sep_s[field, index], lag_row)
        lag_row = jnp.where(lane == FIELD_LANES * field + seps, 0, lag_row)

    def lags_of(field):
        of_field = (lane >= FIELD_LANES * field) & (lane < FIELD_LANES * (field + 1))
        return jnp.where(of_field, lag_row, -1)

    lags_x, lags_y = lags_of(0), lags_of(1)

    load_w.wait()
    lags_z = half + 1
    tile_rows = 8

    def z_step(index, carry):
        start = pl.multiple_of(index * tile_rows, tile_rows)
        rows = [w_own[plane, pl.ds(start, tile_rows), :] for plane in range(planes)]
        return tuple(
            carry[lag] + sum(rows[plane] * rows[plane + lag] for plane in range(planes - lag))
            for lag in range(lags_z)
        )

    zero = jnp.zeros((tile_rows, width_y), jnp.float32)
    z_sums = lax.fori_loop(0, width_x // tile_rows, z_step, (zero,) * lags_z)
    row_z = jnp.zeros((1, LANES), jnp.float32)
    for lag in range(lags_z):
        row_z = jnp.where(lag_row == lag, jnp.sum(z_sums[lag]), row_z)
    row_z = jnp.where((lane >= 2 * FIELD_LANES) & (lane < 3 * FIELD_LANES), row_z, 0.0)

    pltpu.make_async_copy(v_hbm, v_own, load_sem.at[2]).wait()

    def arrived(ref, send, recv):
        return pltpu.make_async_remote_copy(
            src_ref=ref,
            dst_ref=ref,
            send_sem=send,
            recv_sem=recv,
            device_id={"gx": chip_first + 1 - core},
            device_id_type=MESH,
        )

    all_u = arrived(u_own, send_sem.at[0], recv_sem.at[0])
    all_v = arrived(v_own, send_sem.at[1], recv_sem.at[1])
    all_d = arrived(u_wide.at[0, :, pl.ds(0, 2)], send_sem.at[2], recv_sem.at[0])
    all_v.wait_recv()
    cells = half * width_x
    wide = v_wide[...].reshape(3 * cells, width_y)
    high, low = split(wide)
    left = (high[: 2 * cells], low[: 2 * cells])
    gram_0 = product(left, left, ((0,), (0,)))
    gram_1 = product(left, (high[cells:], low[cells:]), ((0,), (0,)))
    gram_y = jnp.concatenate([gram_0, gram_1], axis=1)
    rest = lag_sums(gram_y, lags_y, width_y) + row_z

    all_d.wait_recv()
    gram_x = None
    for item in range(quarter):
        for side in range(2):
            theirs = u_wide.at[side, item, pl.ds(2 - 2 * side, 2)]
            arrived(theirs, send_sem.at[0], u_recv.at[side, item]).wait_recv()
            pair = split(u_wide[side, item].reshape(4 * width_x, width_y))
            lower = (pair[0][: 2 * width_x], pair[1][: 2 * width_x])
            term = product(lower, pair, ((1,), (1,)))
            gram_x = term if gram_x is None else gram_x + term
    mine = lag_sums(gram_x, lags_x, 2 * width_x) + rest

    count = n_gx * n_gy
    me = gx * n_gy + gy
    rows[me] = mine

    place = gy * n_gx + gx

    def to_device(step):
        peer = jnp.where(step < place, step, step + 1)
        return pltpu.make_async_remote_copy(
            src_ref=rows.at[me],
            dst_ref=rows.at[me],
            send_sem=row_sem.at[0],
            recv_sem=row_sem.at[1],
            device_id={"gx": lax.rem(peer, n_gx), "gy": peer // n_gx},
            device_id_type=MESH,
        )

    if count <= 64:
        for step in range(count - 1):
            to_device(step).start()
    else:
        lax.fori_loop(0, count - 1, lambda step, _: to_device(step).start(), None)
    all_rows = arrived(rows.at[pl.ds(0, count - 1)], row_sem.at[0], row_sem.at[1])
    for copy in (all_u, all_v, all_d):
        copy.wait_send()
    all_rows.wait_recv()
    total = jnp.sum(rows[...], axis=0)

    for field in range(3):
        base = FIELD_LANES * field
        row = total[:, base : base + seps] / total[:, base + seps : base + seps + 1]
        if field == 2:
            lag = lag_row[:, base : base + seps].astype(jnp.float32)
            row = row * (jnp.float32(planes) / (jnp.float32(planes) - lag))
        out_ref[field : field + 1, :] = row

    all_rows.wait_send()


def local(n_gx, n_gy, u_field, v_field, w_field, sep_x, sep_y, sep_z):
    planes, width_x, width_y = u_field.shape
    quarter, half = planes // 4, planes // 2
    seps = sep_x.shape[0]
    dma = pltpu.SemaphoreType.DMA
    block = (planes, width_x, width_y)
    return pl.pallas_call(
        functools.partial(kernel, n_gx, n_gy),
        out_shape=pltpu.VMEM((3, seps), jnp.float32),
        in_specs=[pl.BlockSpec(memory_space=pl.ANY)] * 6,
        out_specs=pl.BlockSpec(memory_space=pltpu.VMEM),
        scratch_shapes=[
            pltpu.VMEM((quarter, 2, 2, width_x, width_y), jnp.float32),
            pltpu.VMEM(block, jnp.float32),
            pltpu.VMEM(block, jnp.float32),
            pltpu.VMEM((2, quarter, 4, width_x, width_y), jnp.float32),
            pltpu.VMEM((3, half, width_x, width_y), jnp.float32),
            pltpu.SMEM((3, seps), jnp.int32),
            pltpu.VMEM((n_gx * n_gy, 1, LANES), jnp.float32),
            dma((quarter,)),
            dma((3,)),
            dma((1,)),
            dma((3,)),
            dma((2, quarter)),
            dma((2,)),
            dma((2,)),
            pltpu.SemaphoreType.REGULAR((2,)),
            pltpu.SemaphoreType.REGULAR((n_gy // 2,)),
        ],
        compiler_params=pltpu.CompilerParams(collective_id=0, has_side_effects=True),
    )(u_field.reshape(quarter, 2, 2, width_x, width_y), v_field, w_field, sep_x, sep_y, sep_z)


def solution(mesh):
    return jax.shard_map(
        functools.partial(local, mesh.shape["gx"], mesh.shape["gy"]),
        mesh=mesh,
        in_specs=(P(None, "gx", "gy"), P(None, "gx", "gy"), P(None, "gx", "gy"), P(), P(), P()),
        out_specs=P(),
        check_vma=False,
    )
```

```python
import functools

import jax
import jax.numpy as jnp
from jax import lax
from jax.experimental import pallas as pl
from jax.experimental.pallas import tpu as pltpu
from jax.sharding import PartitionSpec as P

MESH = pl.DeviceIdType.MESH
LANES = 128
FIELD_LANES = 32
GUEST_CORE = 0


def split(value):
    high = value.astype(jnp.bfloat16)
    low = (value - high.astype(jnp.float32)).astype(jnp.bfloat16)
    return high, low


def product(left, right, dims):
    dot = functools.partial(
        lax.dot_general, dimension_numbers=(dims, ((), ())), preferred_element_type=jnp.float32
    )
    return dot(left[0], right[0]) + (dot(left[0], right[1]) + dot(left[1], right[0]))


def lag_sums(gram, offset):
    rows, columns = gram.shape
    at = jnp.broadcast_to(offset, (8, LANES)) + lax.broadcasted_iota(jnp.int32, (8, LANES), 0)
    total = None
    for start in range(0, rows, 8):
        index = at + start
        lane = index & (LANES - 1)
        part = jnp.zeros((8, LANES), jnp.float32)
        for column in range(0, columns, LANES):
            piece = jnp.take_along_axis(gram[start : start + 8, column : column + LANES], lane, axis=1)
            part = jnp.where((index >= column) & (index < column + LANES), piece, part)
        total = part if total is None else total + part
    return total


def folded(gram, window):
    total = gram[:LANES, :window]
    for start in range(LANES, gram.shape[0], LANES):
        total = total + gram[start : start + LANES, start : start + window]
    return total


def kernel(
    n_gx, n_gy,
    u_hbm, v_hbm, w_hbm, sep_x_hbm, sep_y_hbm, sep_z_hbm, out_ref,
    u_own, v_own, w_own, u_wide, u_guest, guest_sums, v_wide, sep_s, rows,
    plane_sem, load_sem, sep_sem, send_sem, u_recv, recv_sem, row_sem, line_sem, pair_sem,
):
    planes, width_x, width_y = v_own.shape
    seps = sep_s.shape[1]
    quarter, half = planes // 4, planes // 2
    SHARED = (1, quarter - 1, 1)
    gx, gy = lax.axis_index("gx"), lax.axis_index("gy")
    core, parity = lax.rem(gx, 2), lax.rem(gy, 2)
    chip_first = gx - core

    load_u = [
        pltpu.make_async_copy(u_hbm.at[item], u_own.at[item], plane_sem.at[item])
        for item in range(quarter)
    ]
    load_v = pltpu.make_async_copy(v_hbm, v_own, load_sem.at[0])
    load_w = pltpu.make_async_copy(w_hbm, w_own, load_sem.at[1])
    for copy in load_u:
        copy.start()
    load_v.start()

    chip, chips = gx // 2, n_gx // 2
    first, last = chip == 0, chip == chips - 1
    near = gy + 1 - 2 * parity
    far_to = lax.rem(gy + n_gy - 2 + 4 * parity, n_gy)
    far_from = lax.rem(gy + n_gy + 2 - 4 * parity, n_gy)
    barrier = pltpu.get_barrier_semaphore()

    def greet(semaphore, **device):
        pl.semaphore_signal(semaphore, inc=1, device_id=device, device_id_type=MESH)

    @pl.when(~first)
    def _():
        greet(barrier, gx=chip_first - 2)
        greet(barrier, gx=chip_first - 1)

    @pl.when(~last)
    def _():
        greet(barrier, gx=chip_first + 2)
        greet(barrier, gx=chip_first + 3)

    gives, takes = gy == n_gy - 1, (gy == 0) & (core == GUEST_CORE)

    @pl.when(takes)
    def _():
        greet(barrier, gx=chip_first, gy=n_gy - 1)
        greet(barrier, gx=chip_first + 1, gy=n_gy - 1)

    greet(barrier, gx=chip_first + 1 - core)
    greet(barrier, gy=near)
    greet(barrier, gy=far_from)
    load_w.start()
    sep_loads = [
        pltpu.make_async_copy(ref, sep_s.at[index], sep_sem.at[0])
        for index, ref in enumerate((sep_x_hbm, sep_y_hbm, sep_z_hbm))
    ]
    places = []
    for side in range(2):
        places.append(pltpu.make_async_copy(
            u_hbm.at[:, side, core],
            u_wide.at[side, :, 2 * side + core],
            load_sem.at[2],
        ))
    places.append(pltpu.make_async_copy(
        v_hbm.at[pl.ds(half * parity, half)], v_wide.at[2 * parity], load_sem.at[2]
    ))
    for copy in places + sep_loads:
        copy.start()

    short = gives & (core == 1)
    part = pl.ds(width_y // 2, width_y // 2)
    kept = pl.ds(0, width_y // 2)

    guest_sums[...] = jnp.zeros_like(guest_sums)

    def u_copy(side, item, other, lanes):
        target = lax.rem(chip_first + (n_gx - 2 if side == 0 else 2), n_gx)
        return pltpu.make_async_remote_copy(
            src_ref=u_own.at[item, side, other, :, lanes],
            dst_ref=u_wide.at[side, item, (2 if side == 0 else 0) + core, :, lanes],
            send_sem=send_sem.at[3 if (side, item, other) == SHARED else 0],
            recv_sem=u_recv.at[side, item],
            device_id={"gx": target + other},
            device_id_type=MESH,
        )

    def start_copy(side, item, other):
        if (side, item, other) != SHARED:
            u_copy(side, item, other, pl.ds(0, width_y)).start()
            return

        @pl.when(gives)
        def _():
            u_copy(side, item, other, kept).start()

        @pl.when(~(gives | takes))
        def _():
            u_copy(side, item, other, pl.ds(0, width_y)).start()

    def arrived(ref, send, recv):
        return pltpu.make_async_remote_copy(
            src_ref=ref,
            dst_ref=ref,
            send_sem=send,
            recv_sem=recv,
            device_id={"gx": chip_first + 1 - core},
            device_id_type=MESH,
        )

    give = pltpu.make_async_remote_copy(
        src_ref=u_own.at[quarter - 1, 1, 1, :, part],
        dst_ref=u_guest.at[core],
        send_sem=send_sem.at[3],
        recv_sem=recv_sem.at[2],
        device_id={"gx": chip_first + GUEST_CORE, "gy": 0},
        device_id_type=MESH,
    )
    guest_on = pltpu.make_async_remote_copy(
        src_ref=u_guest.at[pl.ds(0, 2)],
        dst_ref=u_guest.at[pl.ds(2, 2)],
        send_sem=send_sem.at[4],
        recv_sem=recv_sem.at[3],
        device_id={"gx": lax.rem(chip_first + 2, n_gx) + GUEST_CORE},
        device_id_type=MESH,
    )
    d_copies = []
    for side in range(2):
        d_copies.append(pltpu.make_async_remote_copy(
            src_ref=u_own.at[:, side, 1 - core],
            dst_ref=u_wide.at[side, :, 2 * side + core],
            send_sem=send_sem.at[2],
            recv_sem=recv_sem.at[0],
            device_id={"gx": chip_first + 1 - core},
            device_id_type=MESH,
        ))
    v_copies = []
    for item in range(half):
        v_copies.append(pltpu.make_async_remote_copy(
            src_ref=v_own.at[half * (1 - parity) + item],
            dst_ref=v_wide.at[1, item],
            send_sem=send_sem.at[1],
            recv_sem=recv_sem.at[1],
            device_id={"gy": near},
            device_id_type=MESH,
        ))
        v_copies.append(pltpu.make_async_remote_copy(
            src_ref=v_own.at[half * parity + item],
            dst_ref=v_wide.at[2 - 2 * parity, item],
            send_sem=send_sem.at[1],
            recv_sem=recv_sem.at[1],
            device_id={"gy": far_to},
            device_id_type=MESH,
        ))

    for copy in load_u:
        copy.wait()
    inner = jnp.where(first, 0, 2) + jnp.where(last, 0, 2)
    pl.semaphore_wait(barrier, inner + jnp.where(gives, 4, 3))

    def start_u(side, other, at_end):
        wraps = first if side == 0 else last

        @pl.when(wraps if at_end else ~wraps)
        def _():
            for item in range(quarter):
                start_copy(side, item, other)

    ends = first | last
    for side in range(2):
        start_u(side, 0, False)
    @pl.when(~ends)
    def _():
        for item in range(quarter):
            for side in range(2):
                start_copy(side, item, 1)
    @pl.when(gives)
    def _():
        give.start()

    load_v.wait()
    for copy in v_copies + d_copies:
        copy.start()

    up, down = line_sem.at[0], line_sem.at[1]

    @pl.when(chip == 1)
    def _():
        greet(up, gx=gx + 2)

    @pl.when(chip == chips - 2)
    def _():
        greet(down, gx=gx - 2)

    @pl.when(chip >= 2)
    def _():
        pl.semaphore_wait(up, 1)

    @pl.when((chip >= 2) & (chip <= chips - 2))
    def _():
        greet(up, gx=gx + 2)

    @pl.when(chip <= chips - 3)
    def _():
        pl.semaphore_wait(down, 1)

    @pl.when((chip >= 1) & (chip <= chips - 3))
    def _():
        greet(down, gx=gx - 2)

    @pl.when(ends)
    def _():
        for other in range(2):
            for side in range(2):
                start_u(side, other, True)
        for side in range(2):
            start_u(side, 1, False)

    @pl.when(takes)
    def _():
        arrived(u_guest.at[pl.ds(0, 2)], send_sem.at[3], recv_sem.at[2]).wait_recv()
        guest_on.start()
        u_copy(*SHARED, pl.ds(0, width_y)).start()

    greet(pair_sem.at[0], gy=near)
    pl.semaphore_wait(pair_sem.at[0], 1)
    for hop in range(1, n_gy // 2):
        greet(pair_sem.at[hop], gy=far_from)
        pl.semaphore_wait(pair_sem.at[hop], 1)


    pltpu.make_async_copy(sep_s, sep_s, sep_sem.at[0]).wait()
    lane = lax.broadcasted_iota(jnp.int32, (1, LANES), 1)
    lag_row = jnp.full((1, LANES), -1, jnp.int32)
    for field in range(3):
        for index in range(seps):
            lag_row = jnp.where(lane == FIELD_LANES * field + index, sep_s[field, index], lag_row)
        lag_row = jnp.where(lane == FIELD_LANES * field + seps, 0, lag_row)

    def lags_of(field):
        of_field = (lane >= FIELD_LANES * field) & (lane < FIELD_LANES * (field + 1))
        return jnp.where(of_field, lag_row, -1)

    lags_x, lags_y = lags_of(0), lags_of(1)

    load_w.wait()
    lags_z = half + 1
    tile_rows = 8

    def z_step(index, carry):
        start = pl.multiple_of(index * tile_rows, tile_rows)
        rows = [w_own[plane, pl.ds(start, tile_rows), :] for plane in range(planes)]
        return tuple(
            carry[lag] + sum(rows[plane] * rows[plane + lag] for plane in range(planes - lag))
            for lag in range(lags_z)
        )

    zero = jnp.zeros((tile_rows, width_y), jnp.float32)
    z_sums = lax.fori_loop(0, width_x // tile_rows, z_step, (zero,) * lags_z)
    row_z = jnp.zeros((1, LANES), jnp.float32)
    for lag in range(lags_z):
        row_z = jnp.where(lag_row == lag, jnp.sum(z_sums[lag]), row_z)
    row_z = jnp.where((lane >= 2 * FIELD_LANES) & (lane < 3 * FIELD_LANES), row_z, 0.0)

    pltpu.make_async_copy(v_hbm, v_own, load_sem.at[2]).wait()

    all_u = arrived(v_own.at[pl.ds(0, planes - 1)], send_sem.at[0], recv_sem.at[0])
    all_v = arrived(v_own, send_sem.at[1], recv_sem.at[1])
    all_d = arrived(u_wide.at[0, :, pl.ds(0, 2)], send_sem.at[2], recv_sem.at[0])
    all_v.wait_recv()
    cells = half * width_x
    wide = v_wide[...].reshape(3 * cells, width_y)
    high, low = split(wide)
    left = (high[: 2 * cells], low[: 2 * cells])
    gram_0 = product(left, left, ((0,), (0,)))
    gram_1 = product(left, (high[cells:], low[cells:]), ((0,), (0,)))
    gram_y = jnp.concatenate([gram_0, gram_1], axis=1)
    sums_y = jnp.where(lags_y < 0, 0.0, lag_sums(folded(gram_y, width_y + LANES), lags_y))
    row_z = row_z + jnp.sum(sums_y, axis=0, keepdims=True)

    all_d.wait_recv()
    pair_x = 2 * width_x
    column = lax.broadcasted_iota(jnp.int32, (1, width_y), 1)
    keep = (column < width_y // 2) | ~short

    def block(side, item, slot):
        cells = u_wide[side, item, slot : slot + 2].reshape(pair_x, width_y)
        return split(jnp.where(keep, cells, 0.0) if (side, item) == SHARED[:2] else cells)

    by_rows = ((1,), (1,))
    def add(total, term):
        return term if total is None else total + term

    gram = None
    for side in range(2):
        for item in range(quarter):
            own = block(side, item, 2 * side)
            gram = add(gram, product(own, own, by_rows))
    sums_x = lag_sums(gram, lags_x)

    gram = None
    for item in range(quarter):
        for side in range(2):
            own = block(side, item, 2 * side)
            recv = u_recv.at[side, item]
            whole = arrived(u_wide.at[side, item, pl.ds(2 - 2 * side, 2)], send_sem.at[0], recv)
            if (side, item) == SHARED[:2]:
                @pl.when(short)
                def _():
                    arrived(u_guest.at[pl.ds(0, 2)], send_sem.at[0], recv).wait_recv()

                @pl.when(~short)
                def _():
                    whole.wait_recv()
            else:
                whole.wait_recv()
            theirs = block(side, item, 2 - 2 * side)
            lower, upper = (own, theirs) if side == 0 else (theirs, own)
            gram = add(gram, product(lower, upper, by_rows))
    sums_x = sums_x + lag_sums(gram, lags_x - pair_x)

    @pl.when(takes)
    def _():
        guest_on.wait_recv()
        lower = split(u_guest[2:].reshape(pair_x, width_y // 2))
        upper = split(u_guest[:2].reshape(pair_x, width_y // 2))
        guest_sums[...] = lag_sums(product(upper, upper, by_rows), lags_x) + lag_sums(
            product(lower, upper, by_rows), lags_x - pair_x
        )

    sums_x = sums_x + guest_sums[...]
    mine = jnp.sum(jnp.where(lags_x < 0, 0.0, sums_x), axis=0, keepdims=True) + row_z

    count = n_gx * n_gy
    me = gx * n_gy + gy
    rows[me] = mine

    place = gy * n_gx + gx

    def to_device(step):
        peer = jnp.where(step < place, step, step + 1)
        return pltpu.make_async_remote_copy(
            src_ref=rows.at[me],
            dst_ref=rows.at[me],
            send_sem=row_sem.at[0],
            recv_sem=row_sem.at[1],
            device_id={"gx": lax.rem(peer, n_gx), "gy": peer // n_gx},
            device_id_type=MESH,
        )

    if count <= 64:
        for step in range(count - 1):
            to_device(step).start()
    else:
        lax.fori_loop(0, count - 1, lambda step, _: to_device(step).start(), None)
    all_rows = arrived(rows.at[pl.ds(0, count - 1)], row_sem.at[0], row_sem.at[1])
    for copy in (all_u, all_v, all_d):
        copy.wait_send()

    arrived(u_guest.at[pl.ds(0, 2)], send_sem.at[3], recv_sem.at[2]).wait_send()

    @pl.when(takes)
    def _():
        guest_on.wait_send()

    all_rows.wait_recv()
    total = jnp.sum(rows[...], axis=0)

    for field in range(3):
        base = FIELD_LANES * field
        row = total[:, base : base + seps] / total[:, base + seps : base + seps + 1]
        if field == 2:
            lag = lag_row[:, base : base + seps].astype(jnp.float32)
            row = row * (jnp.float32(planes) / (jnp.float32(planes) - lag))
        out_ref[field : field + 1, :] = row

    all_rows.wait_send()


def local(n_gx, n_gy, u_field, v_field, w_field, sep_x, sep_y, sep_z):
    planes, width_x, width_y = u_field.shape
    quarter, half = planes // 4, planes // 2
    seps = sep_x.shape[0]
    dma = pltpu.SemaphoreType.DMA
    block = (planes, width_x, width_y)
    return pl.pallas_call(
        functools.partial(kernel, n_gx, n_gy),
        out_shape=pltpu.VMEM((3, seps), jnp.float32),
        in_specs=[pl.BlockSpec(memory_space=pl.ANY)] * 6,
        out_specs=pl.BlockSpec(memory_space=pltpu.VMEM),
        scratch_shapes=[
            pltpu.VMEM((quarter, 2, 2, width_x, width_y), jnp.float32),
            pltpu.VMEM(block, jnp.float32),
            pltpu.VMEM(block, jnp.float32),
            pltpu.VMEM((2, quarter, 4, width_x, width_y), jnp.float32),
            pltpu.VMEM((4, width_x, width_y // 2), jnp.float32),
            pltpu.VMEM((8, LANES), jnp.float32),
            pltpu.VMEM((3, half, width_x, width_y), jnp.float32),
            pltpu.SMEM((3, seps), jnp.int32),
            pltpu.VMEM((n_gx * n_gy, 1, LANES), jnp.float32),
            dma((quarter,)),
            dma((3,)),
            dma((1,)),
            dma((5,)),
            dma((2, quarter)),
            dma((4,)),
            dma((2,)),
            pltpu.SemaphoreType.REGULAR((2,)),
            pltpu.SemaphoreType.REGULAR((n_gy // 2,)),
        ],
        compiler_params=pltpu.CompilerParams(collective_id=0, has_side_effects=True),
    )(u_field.reshape(quarter, 2, 2, width_x, width_y), v_field, w_field, sep_x, sep_y, sep_z)


def solution(mesh):
    return jax.shard_map(
        functools.partial(local, mesh.shape["gx"], mesh.shape["gy"]),
        mesh=mesh,
        in_specs=(P(None, "gx", "gy"), P(None, "gx", "gy"), P(None, "gx", "gy"), P(), P(), P()),
        out_specs=P(),
        check_vma=False,
    )
```
